256 devices in a mesh: row: 16 (over y_hi, x, core), col: 16 (over z, y_lo).
Axes of the slice: x: 4, y: 4 (y_hi: 2, y_lo: 2; y = y_hi * 2 + y_lo), z: 8, core: 2. Of those that a mesh axis runs over, the one named last changes fastest.
Arguments:
- blocks: bfloat16 [16, 16, 368, 128, 128], P('row', 'col'), may hold values from -0.125 to 0.125
- block_rows: int32 [16, 16, 368], P('row', 'col'), may hold values from 0 to 127, as said below
- block_cols: int32 [16, 16, 368], P('row', 'col'), may hold values from 0 to 127
- counts: int32 [16, 16], P('row', 'col'), may hold values from 1 to 368, as said below
- features: bfloat16 [262144, 256], P(('col', 'row')), may hold values from -6 to 6
Outputs:
- aggregated: bfloat16 [262144, 256], P(('row', 'col'))
The draws below stay inside these ranges and needn't reach their ends.
Inputs may be any that keep to these rules, and one draw needn't show every extreme that they name: `block_rows`: within one tile the live slots name distinct pairs of block row and block column. `counts`: some tile holds exactly 368 live blocks in every draw.
All inputs are finite; a program needn't handle non-finite values.
Results may differ from the reference program's by a relative error of at most 0.013.
Values may be sent and summed in bfloat16 or wider, within the bound.
No kernel may reach another device: no remote copies, remote signals or barrier semaphores. Data moves between devices by JAX's collectives and lax.ppermute only.
A program may use at most 128 MiB of HBM per device.

```python
import jax
import jax.numpy as jnp
from jax import lax

F = 256
BS = 128
Q = 8
MAXB = 368
BR = 128
BC = 128
NB = 2048
NODES = 262144
N_ROW = 16
N_COL = 16


def pattern_draw(key):
    base_key = jax.random.fold_in(key, 7)
    slot_key = jax.random.fold_in(base_key, 1)
    count_key = jax.random.fold_in(base_key, 2)
    chosen_key = jax.random.fold_in(base_key, 3)
    tile_total = N_ROW * N_COL
    tile_keys = jax.random.split(slot_key, tile_total)
    slot_ids = jax.vmap(lambda tile_key: jax.random.permutation(tile_key, BR * BC)[:MAXB])(tile_keys)
    slot_ids = slot_ids.astype(jnp.int32).reshape(N_ROW, N_COL, MAXB)
    raw_draw = jax.random.randint(count_key, (tile_total,), 0, MAXB + 1, dtype=jnp.int32)
    tile_counts = jnp.maximum(raw_draw * raw_draw // MAXB, 1)
    chosen_tile = jax.random.randint(chosen_key, (), 0, tile_total, dtype=jnp.int32)
    tile_counts = jnp.where(jnp.arange(tile_total, dtype=jnp.int32) == chosen_tile, MAXB, tile_counts)
    return (slot_ids // BC, slot_ids % BC, tile_counts.reshape(N_ROW, N_COL).astype(jnp.int32))


def draw_block_rows(key, part):
    return pattern_draw(key)[0]


def draw_block_cols(key, part):
    return pattern_draw(key)[1]


def draw_counts(key, part):
    return pattern_draw(key)[2]


def level_of(stream_key, extent, pieces, smallest, top_value):
    def one(position, shards_of):
        draws = jax.random.uniform(jax.random.fold_in(jax.random.fold_in(stream_key, 6), position), (shards_of,), jnp.float32, smallest / len(pieces), top_value / len(pieces))
        return jnp.repeat(jnp.exp(draws), extent[position] // shards_of).reshape((-1,) + (1,) * (len(extent) - position - 1))

    factor_of = one(*pieces[0])
    for cut in pieces[1:]:
        factor_of = factor_of * one(*cut)
    return factor_of


def noise(key, shape, spread, limit, pieces=(), kind=jnp.bfloat16):
    result = jax.random.normal(key, shape, jnp.float32) * spread
    if len(pieces) > 0:
        result = level_of(key, shape, pieces, -0.22, 0.18) * result
    return jnp.clip(result, min=-limit, max=limit).astype(kind)


def setup_inputs(seed: int = 0) -> dict:
    seeds = jax.random.split(jax.random.key(seed), 6)
    return {
        "blocks": noise(seeds[0], (N_ROW, N_COL, MAXB, BS, BS), (BS * MAXB // (3 * Q)) ** -0.5, 0.125, ((0, 16), (1, 16))),
        "block_rows": draw_block_rows(jax.random.fold_in(seeds[5], 71), 0),
        "block_cols": draw_block_cols(jax.random.fold_in(seeds[5], 71), 0),
        "counts": draw_counts(jax.random.fold_in(seeds[5], 71), 0),
        "features": noise(seeds[4], (NODES, F), 1.0, 6.0, ((0, 256),)),
    }


def reference(blocks, block_rows, block_cols, counts, features):
    feature_blocks = features.reshape(NB, BS, F)

    def per_tile(running, tile_index):
        row_panel = tile_index // N_COL
        col_panel = tile_index % N_COL
        tile_blocks = blocks[row_panel, col_panel]
        tile_rows = block_rows[row_panel, col_panel]
        tile_cols = block_cols[row_panel, col_panel]
        live_mask = jnp.arange(MAXB, dtype=jnp.int32) < counts[row_panel, col_panel]
        gathered = feature_blocks[(col_panel * BC + tile_cols).astype(jnp.int32)]
        product = jnp.einsum("gik,gkf->gif", tile_blocks.astype(jnp.float32), gathered.astype(jnp.float32))
        product = jnp.where(live_mask[:, None, None], product, jnp.float32(0.0))
        partial_value = jnp.zeros((BR, BS, F), jnp.float32).at[tile_rows.astype(jnp.int32)].add(product)
        rounded = lax.optimization_barrier(partial_value.astype(jnp.bfloat16)).astype(jnp.float32)
        start = (row_panel * BR).astype(jnp.int32)
        zero = jnp.int32(0)
        current = lax.dynamic_slice(running, (start, zero, zero), (BR, BS, F))
        running = lax.dynamic_update_slice(running, current + rounded, (start, zero, zero))
        return running, None

    initial = jnp.zeros((NB, BS, F), jnp.float32)
    running, _ = lax.scan(per_tile, initial, jnp.arange(N_ROW * N_COL, dtype=jnp.int32))
    return running.reshape(NB * BS, F).astype(jnp.bfloat16)
```

```python
import jax
import jax.numpy as jnp
from jax import lax
from jax.experimental import pallas as pl
from jax.experimental.pallas import tpu as pltpu
from jax.sharding import Mesh
from jax.sharding import PartitionSpec as P


ROW = ("yh", "x", "c")
COL = ("z", "yl")
GROUP = 16


def shift(array, axis, step):
    n = lax.axis_size(axis)
    return lax.ppermute(array, axis, [(i, (i + step) % n) for i in range(n)])


def tile_product(blocks, rows, cols, count, pieces, places):
    bs, width = pieces[0].shape[1:]
    n_pieces, n_rows, n_cols = len(pieces), 128, 128

    def body(count_ref, rows_ref, cols_ref, blocks_ref, *rest):
        piece_refs, out_ref = rest[:n_pieces], rest[n_pieces]
        acc, panel, weights, staged, piece_sem, weight_sem, out_sem = rest[n_pieces + 1 :]

        def weight_copy(group, slot):
            return pltpu.make_async_copy(
                blocks_ref.at[pl.ds(group * GROUP, GROUP)], weights.at[slot], weight_sem.at[slot]
            )

        def out_copy(part, slot):
            return pltpu.make_async_copy(staged.at[slot], out_ref.at[pl.ds(part * 8, 8)], out_sem.at[slot])

        piece_copies = [
            pltpu.make_async_copy(ref, panel.at[pl.ds(place, piece.shape[0])], piece_sem.at[i])
            for i, (ref, piece, place) in enumerate(zip(piece_refs, pieces, places))
        ]
        for copy in piece_copies:
            copy.start()
        weight_copy(0, 0).start()

        def clear(i, _):
            acc[i] = jnp.zeros((bs, width), jnp.float32)
            return 0

        lax.fori_loop(0, n_rows + 1, clear, 0)
        for copy in piece_copies:
            copy.wait()
        groups = (count_ref[0] + GROUP - 1) // GROUP

        def one_group(group, _):
            slot = lax.rem(group, 2)

            @pl.when(group + 1 < groups)
            def _():
                weight_copy(group + 1, 1 - slot).start()

            weight_copy(group, slot).wait()
            for i in range(GROUP):
                row = rows_ref[group * GROUP + i]
                col = cols_ref[group * GROUP + i]
                acc[row] += jnp.dot(weights[slot, i], panel[col], preferred_element_type=jnp.float32)
            return 0

        lax.fori_loop(0, groups, one_group, 0)

        def emit(part, _):
            slot = lax.rem(part, 2)

            @pl.when(part >= 2)
            def _():
                out_copy(part - 2, slot).wait()

            for i in range(8):
                staged[slot, i] = acc[part * 8 + i].astype(jnp.bfloat16)
            out_copy(part, slot).start()
            return 0

        parts = n_rows // 8
        lax.fori_loop(0, parts, emit, 0)
        out_copy(parts - 2, 0).wait()
        out_copy(parts - 1, 1).wait()

    hbm = pl.BlockSpec(memory_space=pl.ANY)
    smem = pl.BlockSpec(memory_space=pltpu.SMEM)
    return pl.pallas_call(
        body,
        out_shape=jax.ShapeDtypeStruct((n_rows, bs, width), jnp.bfloat16),
        in_specs=[smem, smem, smem, hbm] + [hbm] * n_pieces,
        out_specs=hbm,
        scratch_shapes=[
            pltpu.VMEM((n_rows + 1, bs, width), jnp.float32),
            pltpu.VMEM((n_cols, bs, width), jnp.bfloat16),
            pltpu.VMEM((2, GROUP, bs, bs), jnp.bfloat16),
            pltpu.VMEM((2, 8, bs, width), jnp.bfloat16),
            pltpu.SemaphoreType.DMA((n_pieces,)),
            pltpu.SemaphoreType.DMA((2,)),
            pltpu.SemaphoreType.DMA((2,)),
        ],
        compiler_params=pltpu.CompilerParams(vmem_limit_bytes=50 * 2**20),
        name="tile_product",
    )(count, rows, cols, blocks, *pieces)


def gather_panel(own):
    got = []

    def around_x(part, dyh, at):
        half = part.shape[0] // 2
        before = shift(part, "x", 1)
        after = shift(part, "x", -1)
        far_low = shift(before[:half], "x", 1)
        far_high = shift(after[half:], "x", -1)
        return [(before, dyh, 3, at), (after, dyh, 1, at), (far_low, dyh, 2, at), (far_high, dyh, 2, at + half)]

    first, second = own[:4], own[4:]
    across = shift(second, "yh", 1)
    ring = around_x(first, 0, 0)
    flipped = shift(first, "yh", 1)
    got += [(across, 1, 0, 4), (flipped, 1, 0, 0)] + ring
    got += [(shift(part, "yh", 1), 1, dx, at) for part, _, dx, at in ring]
    got += around_x(second, 0, 4)
    got += around_x(across, 1, 4)
    got.append((own, 0, 0, 0))
    pieces, places = [], []
    for part, dyh, dx, at in got:
        for dc in range(2):
            pieces.append(shift(part, "c", 1) if dc else part)
            places.append(((dyh * 4 + dx) * 2 + dc) * 8 + at)
    return pieces, places


def ring_sum(parts, step):
    order = [7, 6, 5, 4, 3, 2, 1, 0] if step == 1 else [1, 2, 3, 4, 5, 6, 7, 0]
    moving = parts[order[0]]
    for r in order[1:]:
        moving = parts[r] + shift(moving, "z", step)
    return moving


def on_device(blocks, block_rows, block_cols, counts, features):
    bs = blocks.shape[-1]
    width = features.shape[1]
    yh, x, c = (lax.axis_index(name) for name in ROW)
    z, yl = (lax.axis_index(name) for name in COL)
    rows, cols, count = block_rows[0, 0], block_cols[0, 0], counts[0]
    live = jnp.arange(rows.shape[0], dtype=jnp.int32) < count[0]
    owner = rows // 8
    ahead = ((owner // 2 - z) % 8) * 2 + jnp.bitwise_xor(owner % 2, yl)
    rows = jnp.where(live, ahead * 8 + rows % 8, 128)
    holder = cols // 8
    distance = (
        jnp.bitwise_xor(holder // 8, yh) * 8 + ((holder // 2 - x) % 4) * 2 + jnp.bitwise_xor(holder % 2, c)
    )
    cols = distance * 8 + cols % 8
    pieces, places = gather_panel(features.reshape(-1, bs, width))
    partial = tile_product(blocks[0, 0], rows, cols, count, pieces, places)
    partial = partial.reshape(8, 2, 8, bs, width)

    z_first = []
    for at in (0, 2):
        mine = ring_sum([partial[r, 0, at : at + 2] for r in range(8)], 1)
        other = ring_sum([partial[r, 1, at : at + 2] for r in range(8)], -1)
        z_first.append((mine, other))
    y_first = []
    for at, step in ((4, 1), (6, -1)):
        joined = [partial[r, 0, at : at + 2] + shift(partial[r, 1, at : at + 2], "yl", 1) for r in range(8)]
        y_first.append(ring_sum(joined, step))
    done = [mine + shift(other, "yl", 1) for mine, other in z_first] + y_first
    return jnp.concatenate(done, 0).reshape(-1, width)


def solution(mesh):
    finer = Mesh(mesh.devices.reshape(2, 4, 2, 8, 2), ROW + COL)
    placed = (
        P(ROW, COL, None, None, None),
        P(ROW, COL, None),
        P(ROW, COL, None),
        P(ROW, COL),
        P(COL + ROW, None),
    )
    return jax.shard_map(
        on_device, mesh=finer, in_specs=placed, out_specs=P(ROW + COL, None), check_vma=False
    )
```

```python
import jax
import jax.numpy as jnp
from jax import lax
from jax.experimental import pallas as pl
from jax.experimental.pallas import tpu as pltpu
from jax.sharding import Mesh
from jax.sharding import PartitionSpec as P


ROW = ("yh", "x", "c")
COL = ("z", "yl")
GROUP = 16
BUFFERS = 4
LATE = 4
EARLY = 8 - LATE


def shift(array, axis, step):
    n = lax.axis_size(axis)
    return lax.ppermute(array, axis, [(i, (i + step) % n) for i in range(n)])


def tile_product(blocks, packed, span, pieces, places, first_row, out_rows):
    bs, width = pieces[0].shape[1:]
    n_pieces, n_rows, n_cols, n_outs = len(pieces), sum(out_rows), 128, len(out_rows)
    part_rows = 8

    def body(span_ref, packed_ref, blocks_ref, *rest):
        piece_refs, out_refs = rest[:n_pieces], rest[n_pieces : n_pieces + n_outs]
        acc, panel, weights, staged, piece_sem, weight_sem, out_sem = rest[n_pieces + n_outs :]
        start, stop = span_ref[0], span_ref[1]
        groups = (stop - start + GROUP - 1) // GROUP

        def weight_copies(group):
            slot = lax.rem(group, BUFFERS)
            return [
                pltpu.make_async_copy(
                    blocks_ref.at[packed_ref[start + group * GROUP + i] & 511],
                    weights.at[slot, i],
                    weight_sem.at[slot, i],
                )
                for i in range(GROUP)
            ]

        def fetch(group):
            @pl.when(group < groups)
            def _():
                for copy in weight_copies(group):
                    copy.start()

        piece_copies = [
            pltpu.make_async_copy(ref, panel.at[pl.ds(place, piece.shape[0])], piece_sem.at[i])
            for i, (ref, piece, place) in enumerate(zip(piece_refs, pieces, places))
        ]
        for copy in piece_copies:
            copy.start()
        for group in range(BUFFERS - 1):
            fetch(group)

        def clear(i, _):
            acc[i] = jnp.zeros((bs, width), jnp.float32)
            return 0

        lax.fori_loop(0, n_rows + 1, clear, 0)
        for copy in piece_copies:
            copy.wait()

        def one_group(group, _):
            slot = lax.rem(group, BUFFERS)
            fetch(group + BUFFERS - 1)
            for copy in weight_copies(group):
                copy.wait()
            for i in range(GROUP):
                entry = packed_ref[start + group * GROUP + i]
                row = jnp.minimum((entry >> 16) - first_row, n_rows)
                col = (entry >> 9) & 127
                acc[row] += jnp.dot(weights[slot, i], panel[col], preferred_element_type=jnp.float32)
            return 0

        lax.fori_loop(0, groups, one_group, 0)
        base = 0
        for out_ref, rows in zip(out_refs, out_rows):

            def out_copy(part, slot, out_ref=out_ref):
                return pltpu.make_async_copy(
                    staged.at[slot], out_ref.at[pl.ds(part * part_rows, part_rows)], out_sem.at[slot]
                )

            def emit(part, _, base=base, out_copy=out_copy):
                slot = lax.rem(part, 2)

                @pl.when(part >= 2)
                def _():
                    out_copy(part - 2, slot).wait()

                for i in range(part_rows):
                    staged[slot, i] = acc[base + part * part_rows + i].astype(jnp.bfloat16)
                out_copy(part, slot).start()
                return 0

            parts = rows // part_rows
            lax.fori_loop(0, parts, emit, 0)
            out_copy(parts - 2, (parts - 2) % 2).wait()
            out_copy(parts - 1, (parts - 1) % 2).wait()
            base += rows

    hbm = pl.BlockSpec(memory_space=pl.ANY)
    smem = pl.BlockSpec(memory_space=pltpu.SMEM)
    return pl.pallas_call(
        body,
        out_shape=[jax.ShapeDtypeStruct((rows, bs, width), jnp.bfloat16) for rows in out_rows],
        in_specs=[smem, smem, hbm] + [hbm] * n_pieces,
        out_specs=[hbm] * n_outs,
        scratch_shapes=[
            pltpu.VMEM((n_rows + 1, bs, width), jnp.float32),
            pltpu.VMEM((n_cols, bs, width), jnp.bfloat16),
            pltpu.VMEM((BUFFERS, GROUP, bs, bs), jnp.bfloat16),
            pltpu.VMEM((2, part_rows, bs, width), jnp.bfloat16),
            pltpu.SemaphoreType.DMA((n_pieces,)),
            pltpu.SemaphoreType.DMA((BUFFERS, GROUP)),
            pltpu.SemaphoreType.DMA((2,)),
        ],
        compiler_params=pltpu.CompilerParams(vmem_limit_bytes=59 * 2**20),
        cost_estimate=pl.CostEstimate(
            flops=n_rows * 3 * 2 * bs * bs * width, bytes_accessed=30 * 2**20, transcendentals=0
        ),
        name="tile_product",
    )(span, packed, blocks, *pieces)


def gather_panel(own):
    half = own.shape[0] // 2
    got = [(own, 0, 0, 0)]
    across = shift(own, "yh", 1)
    got.append((across, 1, 0, 0))
    for part, dyh in ((own, 0), (across, 1)):
        before = shift(part, "x", 1)
        after = shift(part, "x", -1)
        far_low = shift(before[:half], "x", 1)
        far_high = shift(after[half:], "x", -1)
        got += [(before, dyh, 3, 0), (after, dyh, 1, 0), (far_low, dyh, 2, 0), (far_high, dyh, 2, half)]
    pieces, places = [], []
    for part, dyh, dx, at in got:
        for dc in range(2):
            pieces.append(shift(part, "c", 1) if dc else part)
            places.append(((dyh * 4 + dx) * 2 + dc) * 8 + at)
    return pieces, places


def sort_slots(rows, cols, live, total):
    slots = jnp.arange(rows.shape[0], dtype=jnp.int32)
    key = jnp.where(live, rows, 128) * 512 + slots
    rank = jnp.sum((key[None, :] < key[:, None]).astype(jnp.int32), axis=1)
    entry = slots + 512 * cols + 65536 * jnp.where(live, rows, 128) - 65536 * 128
    places = jnp.arange(total, dtype=jnp.int32)
    picked = jnp.where(rank[:, None] == places[None, :], entry[:, None], 0)
    return jnp.sum(picked, axis=0) + 65536 * 128


def on_device(blocks, block_rows, block_cols, counts, features):
    bs = blocks.shape[-1]
    width = features.shape[1]
    yh, x, c = (lax.axis_index(name) for name in ROW)
    yl = lax.axis_index("yl")
    rows, cols, count = block_rows[0, 0], block_cols[0, 0], counts[0, 0]
    live = jnp.arange(rows.shape[0], dtype=jnp.int32) < count
    owner, within = rows // 8, rows % 8
    to_z, away = owner // 2, jnp.bitwise_xor(owner % 2, yl)
    early_row = (to_z * 2 + away) * EARLY + within
    late_row = 16 * EARLY + (away * 8 + to_z) * LATE + within - EARLY
    is_early = within < EARLY
    rows = jnp.where(is_early, early_row, late_row)
    n_early = jnp.sum((live & is_early).astype(jnp.int32))
    holder = cols // 8
    distance = (
        jnp.bitwise_xor(holder // 8, yh) * 8 + ((holder // 2 - x) % 4) * 2 + jnp.bitwise_xor(holder % 2, c)
    )
    packed = sort_slots(rows, distance * 8 + cols % 8, live, rows.shape[0] + GROUP)
    pieces, places = gather_panel(features.reshape(-1, bs, width))

    early_span = jnp.stack([jnp.int32(0), n_early])
    late_span = jnp.stack([n_early, count])
    (early,) = tile_product(blocks[0, 0], packed, early_span, pieces, places, 0, [16 * EARLY])
    keep, send = tile_product(
        blocks[0, 0], packed, late_span, pieces, places, 16 * EARLY, [8 * LATE, 8 * LATE]
    )
    early = lax.psum_scatter(early, "z", scatter_dimension=0, tiled=True)
    late = lax.psum_scatter(keep + shift(send, "yl", 1), "z", scatter_dimension=0, tiled=True)
    early = early[:EARLY] + shift(early[EARLY:], "yl", 1)
    return jnp.concatenate([early, late], 0).reshape(-1, width)


def solution(mesh):
    finer = Mesh(mesh.devices.reshape(2, 4, 2, 8, 2), ROW + COL)
    placed = (
        P(ROW, COL, None, None, None),
        P(ROW, COL, None),
        P(ROW, COL, None),
        P(ROW, COL),
        P(COL + ROW, None),
    )
    return jax.shard_map(
        on_device, mesh=finer, in_specs=placed, out_specs=P(ROW + COL, None), check_vma=False
    )
```

```python
import jax
import jax.numpy as jnp
from jax import lax
from jax.experimental import pallas as pl
from jax.experimental.pallas import tpu as pltpu
from jax.sharding import Mesh
from jax.sharding import PartitionSpec as P


ROW = ("yh", "x", "c")
COL = ("z", "yl")
GROUP = 16
BUFFERS = 4
LATE = 3
EARLY = 8 - LATE


def shift(array, axis, step):
    n = lax.axis_size(axis)
    return lax.ppermute(array, axis, [(i, (i + step) % n) for i in range(n)])


def tile_product(blocks, packed, span, pieces, places, first_row, n_rows, outs):
    bs, width = pieces[0].shape[1:]
    n_pieces, n_cols = len(pieces), 128
    in_order = outs is None
    if in_order:
        shapes, stage = [(n_rows, width)], (8, width)
    else:
        shapes = [(sum(seg[3] * seg[6] for seg in out), out[0][1]) for out in outs]
        stage = (outs[0][0][3], outs[0][0][1])
    n_outs = len(shapes)

    def body(span_ref, packed_ref, blocks_ref, *rest):
        piece_refs, out_refs = rest[:n_pieces], rest[n_pieces : n_pieces + n_outs]
        acc, panel, weights, staged, piece_sem, weight_sem, out_sem = rest[n_pieces + n_outs :]
        start, stop = span_ref[0], span_ref[1]
        groups = (stop - start + GROUP - 1) // GROUP

        def weight_copies(group):
            slot = lax.rem(group, BUFFERS)
            return [
                pltpu.make_async_copy(
                    blocks_ref.at[packed_ref[start + group * GROUP + i] & 511],
                    weights.at[slot, i],
                    weight_sem.at[slot, i],
                )
                for i in range(GROUP)
            ]

        def fetch(group):
            @pl.when(group < groups)
            def _():
                for copy in weight_copies(group):
                    copy.start()

        piece_copies = [
            pltpu.make_async_copy(ref, panel.at[pl.ds(place, piece.shape[0])], piece_sem.at[i])
            for i, (ref, piece, place) in enumerate(zip(piece_refs, pieces, places))
        ]
        for copy in piece_copies:
            copy.start()
        for group in range(BUFFERS - 1):
            fetch(group)

        def clear(i, _):
            acc[i] = jnp.zeros((bs, width), jnp.float32)
            return 0

        lax.fori_loop(0, n_rows + 1, clear, 0)
        for copy in piece_copies:
            copy.wait()

        def out_copy(out_ref, at, slot):
            return pltpu.make_async_copy(
                staged.at[slot], out_ref.at[pl.ds(at * stage[0], stage[0])], out_sem.at[slot]
            )

        def emit(count, out_ref, at, row, lane):
            slot = lax.rem(count, 2)

            @pl.when(count >= 2)
            def _():
                out_copy(out_ref, at, slot).wait()

            for i in range(stage[0]):
                staged[slot, i] = acc[row + i, :, lane : lane + stage[1]].astype(jnp.bfloat16)
            out_copy(out_ref, at, slot).start()

        def one_group(group, finished):
            slot = lax.rem(group, BUFFERS)
            fetch(group + BUFFERS - 1)
            for copy in weight_copies(group):
                copy.wait()
            for i in range(GROUP):
                entry = packed_ref[start + group * GROUP + i]
                row = jnp.minimum((entry >> 16) - first_row, n_rows)
                col = (entry >> 9) & 127
                acc[row] += jnp.dot(weights[slot, i], panel[col], preferred_element_type=jnp.float32)
            if not in_order:
                return finished
            following = jnp.minimum((packed_ref[start + (group + 1) * GROUP] >> 16) - first_row, n_rows)
            ready = jnp.where(group + 1 < groups, following, n_rows) // stage[0]

            def write(part, _):
                emit(part, out_refs[0], part, part * stage[0], 0)
                return 0

            lax.fori_loop(finished, ready, write, 0)
            return ready

        finished = lax.fori_loop(0, groups, one_group, 0)
        if in_order:

            def write(part, _):
                emit(part, out_refs[0], part, part * stage[0], 0)
                return 0

            lax.fori_loop(finished, n_rows // stage[0], write, 0)
        else:
            written = 0
            for out_ref, out in zip(out_refs, outs):
                at = 0
                for lane, _, row, group_rows, first, step, count in out:

                    def write(i, _, written=written, at=at, out_ref=out_ref, lane=lane, row=row):
                        source = row + group_rows * lax.rem(first + step * i + 8, 8)
                        emit(written + i, out_ref, at + i, source, lane)
                        return 0

                    lax.fori_loop(0, count, write, 0)
                    written, at = written + count, at + count
        for slot in range(2):
            out_copy(out_refs[-1], 0, slot).wait()

    hbm = pl.BlockSpec(memory_space=pl.ANY)
    smem = pl.BlockSpec(memory_space=pltpu.SMEM)
    return pl.pallas_call(
        body,
        out_shape=[jax.ShapeDtypeStruct((rows, bs, lanes), jnp.bfloat16) for rows, lanes in shapes],
        in_specs=[smem, smem, hbm] + [hbm] * n_pieces,
        out_specs=[hbm] * n_outs,
        scratch_shapes=[
            pltpu.VMEM((n_rows + 1, bs, width), jnp.float32),
            pltpu.VMEM((n_cols, bs, width), jnp.bfloat16),
            pltpu.VMEM((BUFFERS, GROUP, bs, bs), jnp.bfloat16),
            pltpu.VMEM((2, stage[0], bs, stage[1]), jnp.bfloat16),
            pltpu.SemaphoreType.DMA((n_pieces,)),
            pltpu.SemaphoreType.DMA((BUFFERS, GROUP)),
            pltpu.SemaphoreType.DMA((2,)),
        ],
        compiler_params=pltpu.CompilerParams(vmem_limit_bytes=59 * 2**20),
        cost_estimate=pl.CostEstimate(
            flops=n_rows * 3 * 2 * bs * bs * width, bytes_accessed=30 * 2**20, transcendentals=0
        ),
        name="tile_product",
    )(span, packed, blocks, *pieces)


def gather_panel(own):
    half = own.shape[0] // 2
    got = [(own, 0, 0, 0)]
    across = shift(own, "yh", 1)
    got.append((across, 1, 0, 0))
    for part, dyh in ((own, 0), (across, 1)):
        before = shift(part, "x", 1)
        after = shift(part, "x", -1)
        far_low = shift(before[:half], "x", 1)
        far_high = shift(after[half:], "x", -1)
        got += [(before, dyh, 3, 0), (after, dyh, 1, 0), (far_low, dyh, 2, 0), (far_high, dyh, 2, half)]
    pieces, places = [], []
    for part, dyh, dx, at in got:
        for dc in range(2):
            pieces.append(shift(part, "c", 1) if dc else part)
            places.append(((dyh * 4 + dx) * 2 + dc) * 8 + at)
    return pieces, places


def sort_slots(rows, cols, live, total):
    slots = jnp.arange(rows.shape[0], dtype=jnp.int32)
    key = jnp.where(live, rows, 128) * 512 + slots
    rank = jnp.sum((key[None, :] < key[:, None]).astype(jnp.int32), axis=1)
    entry = slots + 512 * cols + 65536 * jnp.where(live, rows, 128) - 65536 * 128
    places = jnp.arange(total, dtype=jnp.int32)
    picked = jnp.where(rank[:, None] == places[None, :], entry[:, None], 0)
    return jnp.sum(picked, axis=0) + 65536 * 128


def on_device(blocks, block_rows, block_cols, counts, features):
    bs = blocks.shape[-1]
    width = features.shape[1]
    half = width // 2
    yh, x, c = (lax.axis_index(name) for name in ROW)
    z, yl = (lax.axis_index(name) for name in COL)
    rows, cols, count = block_rows[0, 0], block_cols[0, 0], counts[0, 0]
    live = jnp.arange(rows.shape[0], dtype=jnp.int32) < count
    owner, within = rows // 8, rows % 8
    to_z, away = owner // 2, jnp.bitwise_xor(owner % 2, yl)
    early_row = (to_z * 2 + away) * EARLY + within
    late_row = 16 * EARLY + (away * 8 + (to_z - z) % 8) * LATE + within - EARLY
    is_early = within < EARLY
    rows = jnp.where(is_early, early_row, late_row)
    n_early = jnp.sum((live & is_early).astype(jnp.int32))
    holder = cols // 8
    distance = (
        jnp.bitwise_xor(holder // 8, yh) * 8 + ((holder // 2 - x) % 4) * 2 + jnp.bitwise_xor(holder % 2, c)
    )
    packed = sort_slots(rows, distance * 8 + cols % 8, live, rows.shape[0] + 2 * GROUP)
    pieces, places = gather_panel(features.reshape(-1, bs, width))
    early_span = jnp.stack([jnp.int32(0), n_early])
    late_span = jnp.stack([n_early, count])
    (early,) = tile_product(blocks[0, 0], packed, early_span, pieces, places, 0, 16 * EARLY, None)

    sent = 8 * LATE
    outs = [
        [(0, half, 0, LATE, 7, -1, 8)],
        [(half, half, 0, LATE, 1, 1, 8)],
        [(0, half, sent, LATE, 7, -1, 4)],
        [(half, half, sent, LATE, 1, 1, 4)],
        [(0, half, sent, LATE, 3, -1, 4)],
        [(half, half, sent, LATE, 5, 1, 4)],
    ]
    keep_up, keep_down, *sends = tile_product(
        blocks[0, 0], packed, late_span, pieces, places, 16 * EARLY, 16 * LATE, outs
    )
    early = lax.psum_scatter(early, "z", scatter_dimension=0, tiled=True)
    got = []
    for send in sends:
        got.append(shift(send, "yl", 1))

    def joined(keep, down, i):
        came, at = got[down + 2 * (i // 4)], i % 4
        return keep[i * LATE : (i + 1) * LATE] + came[at * LATE : (at + 1) * LATE]

    up = joined(keep_up, 0, 0)
    down = joined(keep_down, 1, 0)
    for step in range(7):
        up = shift(up, "z", 1)
        down = shift(down, "z", -1)
        up = joined(keep_up, 0, step + 1) + up
        down = joined(keep_down, 1, step + 1) + down
    crossed = shift(early[EARLY:], "yl", 1)
    early = early[:EARLY] + crossed
    late = jnp.concatenate([up, down], 2)
    return jnp.concatenate([early, late], 0).reshape(-1, width)


def solution(mesh):
    finer = Mesh(mesh.devices.reshape(2, 4, 2, 8, 2), ROW + COL)
    placed = (
        P(ROW, COL, None, None, None),
        P(ROW, COL, None),
        P(ROW, COL, None),
        P(ROW, COL),
        P(COL + ROW, None),
    )

    return jax.shard_map(on_device, mesh=finer, in_specs=placed, out_specs=P(ROW + COL, None), check_vma=False)
```

```python
import jax
import jax.numpy as jnp
from jax import lax
from jax.experimental import pallas as pl
from jax.experimental.pallas import tpu as pltpu
from jax.sharding import Mesh
from jax.sharding import PartitionSpec as P


ROW = ("yh", "x", "c")
COL = ("z", "yl")
GROUP = 16
BUFFERS = 4
LATE = 4
EARLY = 8 - LATE
MESSAGES = (2, 3, 3)


def shift(array, axis, step):
    n = lax.axis_size(axis)
    return lax.ppermute(array, axis, [(i, (i + step) % n) for i in range(n)])


def tile_product(blocks, packed, count, core, pieces, places):
    bs, width = pieces[0].shape[1:]
    half = width // 2
    n_pieces, n_cols, n_rows = len(pieces), 128, 128
    late_rows, part_rows = 16 * LATE, 8
    late_parts, parts = late_rows // part_rows, n_rows // part_rows
    lates = []
    for other, row in ((False, 8 * LATE), (True, 8 * LATE), (False, 0), (True, 0)):
        first = 0
        for n in MESSAGES:
            lates.append((other, row, first, n))
            first += n
    shapes = [(n * LATE, bs, half) for *_, n in lates]

    def body(count_ref, core_ref, packed_ref, blocks_ref, *rest):
        piece_refs, out_ref = rest[:n_pieces], rest[n_pieces]
        late_refs = rest[n_pieces + 1 : n_pieces + 1 + len(lates)]
        acc, panel, weights, staged, *rest = rest[n_pieces + 1 + len(lates) :]
        late_staged, (piece_sem, weight_sem, out_sem, late_sem) = rest[: len(lates)], rest[len(lates) :]
        groups = (count_ref[0] + GROUP - 1) // GROUP

        def weight_copies(group):
            slot = lax.rem(group, BUFFERS)
            return [
                pltpu.make_async_copy(
                    blocks_ref.at[packed_ref[group * GROUP + i] & 511],
                    weights.at[slot, i],
                    weight_sem.at[slot, i],
                )
                for i in range(GROUP)
            ]

        def fetch(group):
            @pl.when(group < groups)
            def _():
                for copy in weight_copies(group):
                    copy.start()

        piece_copies = [
            pltpu.make_async_copy(ref, panel.at[pl.ds(place, piece.shape[0])], piece_sem.at[i])
            for i, (ref, piece, place) in enumerate(zip(piece_refs, pieces, places))
        ]
        for copy in piece_copies:
            copy.start()
        for group in range(BUFFERS - 1):
            fetch(group)

        def clear(i, _):
            acc[i] = jnp.zeros((bs, width), jnp.float32)
            return 0

        lax.fori_loop(0, n_rows + 1, clear, 0)
        for copy in piece_copies:
            copy.wait()

        def out_copy(at, slot):
            return pltpu.make_async_copy(
                staged.at[slot], out_ref.at[pl.ds(at * part_rows, part_rows)], out_sem.at[slot]
            )

        def late_copy(i):
            return pltpu.make_async_copy(late_staged[i], late_refs[i], late_sem.at[i])

        def write_late(on_core):
            for i, (other, row, first, n) in enumerate(lates):
                up = other == (on_core == 1)
                lane = 0 if up else half

                def group_of(at, _, i=i, row=row, first=first, up=up, lane=lane):
                    distance = 7 - first - at if up else lax.rem(first + 1 + at, 8)
                    for k in range(LATE):
                        value = acc[row + distance * LATE + k, :, lane : lane + half]
                        late_staged[i][at * LATE + k] = value.astype(jnp.bfloat16)
                    return 0

                lax.fori_loop(0, n, group_of, 0)
                late_copy(i).start()

        def write(part, _):
            @pl.when(jnp.logical_and(part == late_parts - 1, core_ref[0] == 0))
            def _():
                write_late(0)

            @pl.when(jnp.logical_and(part == late_parts - 1, core_ref[0] == 1))
            def _():
                write_late(1)

            @pl.when(part >= late_parts)
            def _():
                at = part - late_parts
                slot = lax.rem(at, 2)

                @pl.when(at >= 2)
                def _():
                    out_copy(at - 2, slot).wait()

                for i in range(part_rows):
                    staged[slot, i] = acc[part * part_rows + i].astype(jnp.bfloat16)
                out_copy(at, slot).start()

            return 0

        def one_group(group, finished):
            slot = lax.rem(group, BUFFERS)
            fetch(group + BUFFERS - 1)
            for copy in weight_copies(group):
                copy.wait()
            for i in range(GROUP):
                entry = packed_ref[group * GROUP + i]
                row = 128 - (entry >> 16)
                col = (entry >> 9) & 127
                acc[row] += jnp.dot(weights[slot, i], panel[col], preferred_element_type=jnp.float32)
            ready = (128 - (packed_ref[(group + 1) * GROUP] >> 16)) // part_rows
            lax.fori_loop(finished, ready, write, 0)
            return ready

        finished = lax.fori_loop(0, groups, one_group, 0)
        lax.fori_loop(finished, parts, write, 0)
        for slot in range(2):
            out_copy(0, slot).wait()
        for i in range(len(lates)):
            late_copy(i).wait()

    anywhere = pl.BlockSpec(memory_space=pl.ANY)
    hbm = pl.BlockSpec(memory_space=pltpu.MemorySpace.HBM)
    smem = pl.BlockSpec(memory_space=pltpu.SMEM)
    early_shape = jax.ShapeDtypeStruct((16 * EARLY, bs, width), jnp.bfloat16)
    return pl.pallas_call(
        body,
        out_shape=[early_shape] + [jax.ShapeDtypeStruct(shape, jnp.bfloat16) for shape in shapes],
        in_specs=[smem, smem, smem, hbm] + [anywhere] * n_pieces,
        out_specs=[hbm] + [anywhere] * len(lates),
        scratch_shapes=[
            pltpu.VMEM((n_rows + 1, bs, width), jnp.float32),
            pltpu.VMEM((n_cols, bs, width), jnp.bfloat16),
            pltpu.VMEM((BUFFERS, GROUP, bs, bs), jnp.bfloat16),
            pltpu.VMEM((2, part_rows, bs, width), jnp.bfloat16),
            *[pltpu.VMEM(shape, jnp.bfloat16) for shape in shapes],
            pltpu.SemaphoreType.DMA((n_pieces,)),
            pltpu.SemaphoreType.DMA((BUFFERS, GROUP)),
            pltpu.SemaphoreType.DMA((2,)),
            pltpu.SemaphoreType.DMA((len(lates),)),
        ],
        compiler_params=pltpu.CompilerParams(vmem_limit_bytes=50 * 2**20),
        cost_estimate=pl.CostEstimate(
            flops=n_rows * 3 * 2 * bs * bs * width, bytes_accessed=30 * 2**20, transcendentals=0
        ),
        name="tile_product",
    )(count, core, packed, blocks, *pieces)


def gather_panel(own):
    half = own.shape[0] // 2
    got = [(own, 0, 0, 0)]
    across = shift(own, "yh", 1)
    got.append((across, 1, 0, 0))
    for part, dyh in ((own, 0), (across, 1)):
        before = shift(part, "x", 1)
        after = shift(part, "x", -1)
        far_low = shift(before[:half], "x", 1)
        far_high = shift(after[half:], "x", -1)
        got += [(before, dyh, 3, 0), (after, dyh, 1, 0), (far_low, dyh, 2, 0), (far_high, dyh, 2, half)]
    pieces, places = [], []
    for part, dyh, dx, at in got:
        for dc in range(2):
            pieces.append(shift(part, "c", 1) if dc else part)
            places.append(((dyh * 4 + dx) * 2 + dc) * 8 + at)
    return pieces, places


def sort_slots(rows, cols, live, total):
    slots = jnp.arange(rows.shape[0], dtype=jnp.int32)
    key = jnp.where(live, rows, 128) * 512 + slots
    rank = jnp.sum((key[None, :] < key[:, None]).astype(jnp.int32), axis=1)
    entry = jnp.where(live, slots + 512 * cols + 65536 * (128 - rows), 0)
    places = jnp.arange(total, dtype=jnp.int32)
    picked = jnp.where(rank[:, None] == places[None, :], entry[:, None], 0)
    return jnp.sum(picked, axis=0)


def flip(array, axes):
    n = 2 ** len(axes)
    return lax.ppermute(array, axes, [(i, n - 1 - i) for i in range(n)])


def on_device(blocks, block_rows, block_cols, counts, features):
    bs = blocks.shape[-1]
    width = features.shape[1]
    yh, x, c = (lax.axis_index(name) for name in ROW)
    z, yl = (lax.axis_index(name) for name in COL)
    rows, cols, count = block_rows[0, 0], block_cols[0, 0], counts[0]
    live = jnp.arange(rows.shape[0], dtype=jnp.int32) < count[0]
    owner, within = rows // 8, rows % 8
    to_z, away = owner // 2, jnp.bitwise_xor(owner % 2, yl)
    early_row = 16 * LATE + (to_z * 2 + away) * EARLY + within - LATE
    late_row = (away * 8 + (to_z - z) % 8) * LATE + within
    rows = jnp.where(within < LATE, late_row, early_row)
    holder = cols // 8
    distance = (
        jnp.bitwise_xor(holder // 8, yh) * 8 + ((holder // 2 - x) % 4) * 2 + jnp.bitwise_xor(holder % 2, c)
    )
    packed = sort_slots(rows, distance * 8 + cols % 8, live, rows.shape[0] + 2 * GROUP)
    pieces, places = gather_panel(features.reshape(-1, bs, width))
    early, *parts = tile_product(
        blocks[0, 0], packed, count, c.reshape(1), pieces, places
    )
    early = lax.psum_scatter(early, "z", scatter_dimension=0, tiled=True)

    n = len(MESSAGES)
    joined = []
    for i in range(n):
        mine = flip(parts[i], ("yl",))
        theirs = flip(parts[n + i], ("c", "yl"))
        kept_theirs = flip(parts[3 * n + i], ("c",))
        shape = (MESSAGES[i], 1, LATE, bs, width // 2)
        both = jnp.concatenate(
            [(parts[2 * n + i] + mine).reshape(shape), (kept_theirs + theirs).reshape(shape)], 1
        )
        both = lax.optimization_barrier(both)
        joined += [both[k] for k in range(MESSAGES[i])]
    moving = joined[0]
    around = [(i, (i + 1) % 8) for i in range(8)] + [(8 + i, 8 + (i - 1) % 8) for i in range(8)]
    for step in range(7):
        moving = lax.ppermute(moving, ("c", "z"), around)
        moving = joined[step + 1] + moving
    other_half = flip(moving[1], ("c",))
    last = flip(early[EARLY:], ("yl",))
    own_half = moving[0]
    low = jnp.where(c == 0, own_half, other_half)
    high = jnp.where(c == 0, other_half, own_half)
    late = jnp.concatenate([low, high], 2)
    return jnp.concatenate([late, early[:EARLY] + last], 0).reshape(-1, width)


def solution(mesh):
    finer = Mesh(mesh.devices.reshape(2, 4, 2, 8, 2), ROW + COL)
    placed = (
        P(ROW, COL, None, None, None),
        P(ROW, COL, None),
        P(ROW, COL, None),
        P(ROW, COL),
        P(COL + ROW, None),
    )

    return jax.shard_map(on_device, mesh=finer, in_specs=placed, out_specs=P(ROW + COL, None), check_vma=False)
```

```python
import jax
import jax.numpy as jnp
from jax import lax
from jax.experimental import pallas as pl
from jax.experimental.pallas import tpu as pltpu
from jax.sharding import Mesh
from jax.sharding import PartitionSpec as P


ROW = ("yh", "x", "c")
COL = ("z", "yl")
GROUP = 16
BUFFERS = 4
LATE = 4
EARLY = 8 - LATE
HOPS = 4


def shift(array, axis, step):
    n = lax.axis_size(axis)
    return lax.ppermute(array, axis, [(i, (i + step) % n) for i in range(n)])


def tile_product(blocks, packed, count, core, pieces, places):
    bs, width = pieces[0].shape[1:]
    n_pieces, n_cols, n_rows = len(pieces), 128, 128
    late_rows, part_rows = 16 * LATE, 8
    late_parts, parts = late_rows // part_rows, n_rows // part_rows
    lates = []
    for row in (8 * LATE, 0):
        for other in range(2):
            lates += [(row, other, hop, LATE if hop else LATE // 2) for hop in range(HOPS)]
        lates.append((row, None, 0, LATE))
    shapes = [(n, bs, width) for *_, n in lates]

    def body(count_ref, core_ref, packed_ref, blocks_ref, *rest):
        piece_refs, out_ref = rest[:n_pieces], rest[n_pieces]
        late_refs = rest[n_pieces + 1 : n_pieces + 1 + len(lates)]
        acc, panel, weights, staged, *rest = rest[n_pieces + 1 + len(lates) :]
        late_staged, (piece_sem, weight_sem, out_sem, late_sem) = rest[: len(lates)], rest[len(lates) :]
        groups = (count_ref[0] + GROUP - 1) // GROUP

        def weight_copies(group):
            slot = lax.rem(group, BUFFERS)
            return [
                pltpu.make_async_copy(
                    blocks_ref.at[packed_ref[group * GROUP + i] & 511],
                    weights.at[slot, i],
                    weight_sem.at[slot, i],
                )
                for i in range(GROUP)
            ]

        def fetch(group):
            @pl.when(group < groups)
            def _():
                for copy in weight_copies(group):
                    copy.start()

        piece_copies = [
            pltpu.make_async_copy(ref, panel.at[pl.ds(place, piece.shape[0])], piece_sem.at[i])
            for i, (ref, piece, place) in enumerate(zip(piece_refs, pieces, places))
        ]
        for copy in piece_copies:
            copy.start()
        for group in range(BUFFERS - 1):
            fetch(group)

        def clear(i, _):
            acc[i] = jnp.zeros((bs, width), jnp.float32)
            return 0

        lax.fori_loop(0, n_rows + 1, clear, 0)
        for copy in piece_copies:
            copy.wait()

        def out_copy(at, slot):
            return pltpu.make_async_copy(
                staged.at[slot], out_ref.at[pl.ds(at * part_rows, part_rows)], out_sem.at[slot]
            )

        def late_copy(i):
            return pltpu.make_async_copy(late_staged[i], late_refs[i], late_sem.at[i])

        def write_late():
            for i, (row, other, hop, n) in enumerate(lates):
                if other is None:
                    distance = skip = 0
                else:
                    down = 1 - core_ref[0] if other else core_ref[0]
                    distance = 4 + hop * (2 * down - 1)
                    skip = 0 if hop else (1 - down) * (LATE // 2)

                def one_row(k, _, i=i, first=row + distance * LATE + skip):
                    late_staged[i][k] = acc[first + k].astype(jnp.bfloat16)
                    return 0

                lax.fori_loop(0, n, one_row, 0)
                late_copy(i).start()

        def write(part, _):
            @pl.when(part == late_parts - 1)
            def _():
                write_late()

            @pl.when(part >= late_parts)
            def _():
                at = part - late_parts
                slot = lax.rem(at, 2)

                @pl.when(at >= 2)
                def _():
                    out_copy(at - 2, slot).wait()

                for i in range(part_rows):
                    staged[slot, i] = acc[part * part_rows + i].astype(jnp.bfloat16)
                out_copy(at, slot).start()

            return 0

        def one_group(group, finished):
            slot = lax.rem(group, BUFFERS)
            fetch(group + BUFFERS - 1)
            for copy in weight_copies(group):
                copy.wait()
            for i in range(GROUP):
                entry = packed_ref[group * GROUP + i]
                row = 128 - (entry >> 16)
                col = (entry >> 9) & 127
                acc[row] += jnp.dot(weights[slot, i], panel[col], preferred_element_type=jnp.float32)
            ready = (128 - (packed_ref[(group + 1) * GROUP] >> 16)) // part_rows
            lax.fori_loop(finished, ready, write, 0)
            return ready

        finished = lax.fori_loop(0, groups, one_group, 0)
        lax.fori_loop(finished, parts, write, 0)
        for slot in range(2):
            out_copy(0, slot).wait()
        for i in range(len(lates)):
            late_copy(i).wait()

    anywhere = pl.BlockSpec(memory_space=pl.ANY)
    hbm = pl.BlockSpec(memory_space=pltpu.MemorySpace.HBM)
    smem = pl.BlockSpec(memory_space=pltpu.SMEM)
    early_shape = jax.ShapeDtypeStruct((16 * EARLY, bs, width), jnp.bfloat16)
    return pl.pallas_call(
        body,
        out_shape=[early_shape] + [jax.ShapeDtypeStruct(shape, jnp.bfloat16) for shape in shapes],
        in_specs=[smem, smem, smem, hbm] + [anywhere] * n_pieces,
        out_specs=[hbm] + [anywhere] * len(lates),
        scratch_shapes=[
            pltpu.VMEM((n_rows + 1, bs, width), jnp.float32),
            pltpu.VMEM((n_cols, bs, width), jnp.bfloat16),
            pltpu.VMEM((BUFFERS, GROUP, bs, bs), jnp.bfloat16),
            pltpu.VMEM((2, part_rows, bs, width), jnp.bfloat16),
            *[pltpu.VMEM(shape, jnp.bfloat16) for shape in shapes],
            pltpu.SemaphoreType.DMA((n_pieces,)),
            pltpu.SemaphoreType.DMA((BUFFERS, GROUP)),
            pltpu.SemaphoreType.DMA((2,)),
            pltpu.SemaphoreType.DMA((len(lates),)),
        ],
        compiler_params=pltpu.CompilerParams(vmem_limit_bytes=59 * 2**20),
        cost_estimate=pl.CostEstimate(
            flops=n_rows * 3 * 2 * bs * bs * width, bytes_accessed=30 * 2**20, transcendentals=0
        ),
        name="tile_product",
    )(count, core, packed, blocks, *pieces)


def gather_panel(own):
    half = own.shape[0] // 2
    got = [(own, 0, 0, 0)]
    across = shift(own, "yh", 1)
    got.append((across, 1, 0, 0))
    for part, dyh in ((own, 0), (across, 1)):
        before = shift(part, "x", 1)
        after = shift(part, "x", -1)
        far_low = shift(before[:half], "x", 1)
        far_high = shift(after[half:], "x", -1)
        got += [(before, dyh, 3, 0), (after, dyh, 1, 0), (far_low, dyh, 2, 0), (far_high, dyh, 2, half)]
    pieces, places = [], []
    for part, dyh, dx, at in got:
        for dc in range(2):
            pieces.append(shift(part, "c", 1) if dc else part)
            places.append(((dyh * 4 + dx) * 2 + dc) * 8 + at)
    return pieces, places


def sort_slots(rows, cols, live, total):
    slots = jnp.arange(rows.shape[0], dtype=jnp.int32)
    key = jnp.where(live, rows, 128) * 512 + slots
    rank = jnp.sum((key[None, :] < key[:, None]).astype(jnp.int32), axis=1)
    entry = jnp.where(live, slots + 512 * cols + 65536 * (128 - rows), 0)
    places = jnp.arange(total, dtype=jnp.int32)
    picked = jnp.where(rank[:, None] == places[None, :], entry[:, None], 0)
    return jnp.sum(picked, axis=0)


def flip(array, axes):
    n = 2 ** len(axes)
    return lax.ppermute(array, axes, [(i, n - 1 - i) for i in range(n)])


def on_device(blocks, block_rows, block_cols, counts, features):
    bs = blocks.shape[-1]
    width = features.shape[1]
    yh, x, c = (lax.axis_index(name) for name in ROW)
    z, yl = (lax.axis_index(name) for name in COL)
    rows, cols, count = block_rows[0, 0], block_cols[0, 0], counts[0]
    live = jnp.arange(rows.shape[0], dtype=jnp.int32) < count[0]
    owner, within = rows // 8, rows % 8
    to_z, away = owner // 2, jnp.bitwise_xor(owner % 2, yl)
    early_row = 16 * LATE + (to_z * 2 + away) * EARLY + within - LATE
    late_row = (away * 8 + (to_z - z) % 8) * LATE + within
    rows = jnp.where(within < LATE, late_row, early_row)
    holder = cols // 8
    distance = (
        jnp.bitwise_xor(holder // 8, yh) * 8 + ((holder // 2 - x) % 4) * 2 + jnp.bitwise_xor(holder % 2, c)
    )
    packed = sort_slots(rows, distance * 8 + cols % 8, live, rows.shape[0] + 2 * GROUP)
    pieces, places = gather_panel(features.reshape(-1, bs, width))
    early, *parts = tile_product(
        blocks[0, 0], packed, count, c.reshape(1), pieces, places
    )
    early = lax.psum_scatter(early, "z", scatter_dimension=0, tiled=True)

    sent, kept = parts[: 2 * HOPS + 1], parts[2 * HOPS + 1 :]
    joined = []
    for hop in range(HOPS):
        mine = flip(sent[hop], ("yl",))
        theirs = flip(sent[HOPS + hop], ("c", "yl"))
        kept_theirs = flip(kept[HOPS + hop], ("c",))
        joined.append(lax.optimization_barrier(jnp.stack([kept[hop] + mine, kept_theirs + theirs])))
    near = flip(sent[2 * HOPS], ("yl",))
    around = [(i, (i + 1) % 8) for i in range(8)] + [(8 + i, 8 + (i - 1) % 8) for i in range(8)]
    moving = joined[0]
    for hop in range(HOPS):
        moving = lax.ppermute(moving, ("c", "z"), around)
        if hop == HOPS - 1:
            break
        if hop == 0:
            below = jnp.pad(moving, ((0, 0), (LATE // 2, 0), (0, 0), (0, 0)))
            above = jnp.pad(moving, ((0, 0), (0, LATE // 2), (0, 0), (0, 0)))
            moving = jnp.where(c == 0, below, above)
        moving = joined[hop + 1] + moving
    other_side = flip(moving[1], ("c",))
    last = flip(early[EARLY:], ("yl",))
    late = moving[0] + other_side + (kept[2 * HOPS] + near)
    return jnp.concatenate([late, early[:EARLY] + last], 0).reshape(-1, width)


def solution(mesh):
    finer = Mesh(mesh.devices.reshape(2, 4, 2, 8, 2), ROW + COL)
    placed = (
        P(ROW, COL, None, None, None),
        P(ROW, COL, None),
        P(ROW, COL, None),
        P(ROW, COL),
        P(COL + ROW, None),
    )

    return jax.shard_map(on_device, mesh=finer, in_specs=placed, out_specs=P(ROW + COL, None), check_vma=False)
```

```python
import jax
import jax.numpy as jnp
from jax import lax
from jax.experimental import pallas as pl
from jax.experimental.pallas import tpu as pltpu
from jax.sharding import Mesh
from jax.sharding import PartitionSpec as P


ROW = ("yh", "x", "c")
COL = ("z", "yl")
GROUP = 16
BUFFERS = 4
LATE = 4
EARLY = 8 - LATE
HOPS = 4


def shift(array, axis, step):
    n = lax.axis_size(axis)
    return lax.ppermute(array, axis, [(i, (i + step) % n) for i in range(n)])


def tile_product(blocks, packed, count, core, pieces, places):
    bs, width = pieces[0].shape[1:]
    n_pieces, n_cols, n_rows = len(pieces), 128, 128
    late_rows, part_rows = 16 * LATE, 8
    late_parts, parts = late_rows // part_rows, n_rows // part_rows
    lates = []
    for row in (8 * LATE, 0):
        for other in range(2):
            lates += [(row, other, hop, LATE if hop else LATE // 2) for hop in range(HOPS)]
        lates.append((row, None, 0, LATE))
    shapes = [(n, bs, width) for *_, n in lates]

    def body(count_ref, core_ref, packed_ref, blocks_ref, *rest):
        piece_refs, out_ref = rest[:n_pieces], rest[n_pieces]
        late_refs = rest[n_pieces + 1 : n_pieces + 1 + len(lates)]
        acc, panel, weights, staged, *rest = rest[n_pieces + 1 + len(lates) :]
        late_staged, (piece_sem, weight_sem, out_sem, late_sem) = rest[: len(lates)], rest[len(lates) :]
        groups = (count_ref[0] + GROUP - 1) // GROUP

        def weight_copies(group):
            slot = lax.rem(group, BUFFERS)
            return [
                pltpu.make_async_copy(
                    blocks_ref.at[packed_ref[group * GROUP + i] & 511],
                    weights.at[slot, i],
                    weight_sem.at[slot, i],
                )
                for i in range(GROUP)
            ]

        def fetch(group):
            @pl.when(group < groups)
            def _():
                for copy in weight_copies(group):
                    copy.start()

        piece_copies = [
            pltpu.make_async_copy(ref, panel.at[pl.ds(place, piece.shape[0])], piece_sem.at[i])
            for i, (ref, piece, place) in enumerate(zip(piece_refs, pieces, places))
        ]
        for copy in piece_copies:
            copy.start()
        for group in range(BUFFERS - 1):
            fetch(group)

        def clear(i, _):
            acc[i] = jnp.zeros((bs, width), jnp.float32)
            return 0

        lax.fori_loop(0, n_rows + 1, clear, 0)
        for copy in piece_copies:
            copy.wait()

        def out_copy(at, slot):
            return pltpu.make_async_copy(
                staged.at[slot], out_ref.at[pl.ds(at * part_rows, part_rows)], out_sem.at[slot]
            )

        def late_copy(i):
            return pltpu.make_async_copy(late_staged[i], late_refs[i], late_sem.at[i])

        def write_late():
            for i, (row, other, hop, n) in enumerate(lates):
                if other is None:
                    distance = skip = 0
                else:
                    down = 1 - core_ref[0] if other else core_ref[0]
                    distance = 4 + hop * (2 * down - 1)
                    skip = 0 if hop else (1 - down) * (LATE // 2)

                def one_row(k, _, i=i, first=row + distance * LATE + skip):
                    late_staged[i][k] = acc[first + k].astype(jnp.bfloat16)
                    return 0

                lax.fori_loop(0, n, one_row, 0)
                late_copy(i).start()

        def write(part, _):
            @pl.when(part == late_parts - 1)
            def _():
                write_late()

            @pl.when(part >= late_parts)
            def _():
                at = part - late_parts
                slot = lax.rem(at, 2)

                @pl.when(at >= 2)
                def _():
                    out_copy(at - 2, slot).wait()

                for i in range(part_rows):
                    staged[slot, i] = acc[part * part_rows + i].astype(jnp.bfloat16)
                out_copy(at, slot).start()

            return 0

        def one_group(group, finished):
            slot = lax.rem(group, BUFFERS)
            fetch(group + BUFFERS - 1)
            for copy in weight_copies(group):
                copy.wait()
            for i in range(GROUP):
                entry = packed_ref[group * GROUP + i]
                row = 128 - (entry >> 16)
                col = (entry >> 9) & 127
                acc[row] += jnp.dot(weights[slot, i], panel[col], preferred_element_type=jnp.float32)
            ready = (128 - (packed_ref[(group + 1) * GROUP] >> 16)) // part_rows
            lax.fori_loop(finished, ready, write, 0)
            return ready

        finished = lax.fori_loop(0, groups, one_group, 0)
        lax.fori_loop(finished, parts, write, 0)
        for slot in range(2):
            out_copy(0, slot).wait()
        for i in range(len(lates)):
            late_copy(i).wait()

    anywhere = pl.BlockSpec(memory_space=pl.ANY)
    hbm = pl.BlockSpec(memory_space=pltpu.MemorySpace.HBM)
    smem = pl.BlockSpec(memory_space=pltpu.SMEM)
    early_shape = jax.ShapeDtypeStruct((16 * EARLY, bs, width), jnp.bfloat16)
    return pl.pallas_call(
        body,
        out_shape=[early_shape] + [jax.ShapeDtypeStruct(shape, jnp.bfloat16) for shape in shapes],
        in_specs=[smem, smem, smem, hbm] + [anywhere] * n_pieces,
        out_specs=[hbm] + [anywhere] * len(lates),
        scratch_shapes=[
            pltpu.VMEM((n_rows + 1, bs, width), jnp.float32),
            pltpu.VMEM((n_cols, bs, width), jnp.bfloat16),
            pltpu.VMEM((BUFFERS, GROUP, bs, bs), jnp.bfloat16),
            pltpu.VMEM((2, part_rows, bs, width), jnp.bfloat16),
            *[pltpu.VMEM(shape, jnp.bfloat16) for shape in shapes],
            pltpu.SemaphoreType.DMA((n_pieces,)),
            pltpu.SemaphoreType.DMA((BUFFERS, GROUP)),
            pltpu.SemaphoreType.DMA((2,)),
            pltpu.SemaphoreType.DMA((len(lates),)),
        ],
        compiler_params=pltpu.CompilerParams(vmem_limit_bytes=59 * 2**20),
        cost_estimate=pl.CostEstimate(
            flops=n_rows * 3 * 2 * bs * bs * width, bytes_accessed=30 * 2**20, transcendentals=0
        ),
        name="tile_product",
    )(count, core, packed, blocks, *pieces)


def gather_panel(own):
    half = own.shape[0] // 2

    def around_x(part, dyh, at):
        middle = part.shape[0] // 2
        before, after = shift(part, "x", 1), shift(part, "x", -1)
        low, high = before[:middle], after[middle:]
        far = [(shift(low, "x", 1), dyh, 2, at), (shift(high, "x", -1), dyh, 2, at + middle)]
        return before, after, low, [(before, dyh, 3, at), (after, dyh, 1, at), *far]

    across = shift(own, "yh", 1)
    _, after, low, near_side = around_x(own, 0, 0)
    got = [(own, 0, 0, 0), (across, 1, 0, 0), *near_side]
    got += [(shift(low, "yh", 1), 1, 3, 0), (shift(after[:half], "yh", 1), 1, 1, 0)]
    got.append((shift(near_side[2][0], "yh", 1), 1, 2, 0))
    got += around_x(across[half:], 1, half)[3]
    pieces, places = [], []
    for part, dyh, dx, at in got:
        for dc in range(2):
            pieces.append(shift(part, "c", 1) if dc else part)
            places.append(((dyh * 4 + dx) * 2 + dc) * 8 + at)
    return pieces, places


def sort_slots(rows, cols, live, total):
    slots = jnp.arange(rows.shape[0], dtype=jnp.int32)
    key = jnp.where(live, rows, 128) * 512 + slots
    rank = jnp.sum((key[None, :] < key[:, None]).astype(jnp.int32), axis=1)
    entry = jnp.where(live, slots + 512 * cols + 65536 * (128 - rows), 0)
    places = jnp.arange(total, dtype=jnp.int32)
    picked = jnp.where(rank[:, None] == places[None, :], entry[:, None], 0)
    return jnp.sum(picked, axis=0)


def flip(array, axes):
    n = 2 ** len(axes)
    return lax.ppermute(array, axes, [(i, n - 1 - i) for i in range(n)])


def on_device(blocks, block_rows, block_cols, counts, features):
    bs = blocks.shape[-1]
    width = features.shape[1]
    yh, x, c = (lax.axis_index(name) for name in ROW)
    z, yl = (lax.axis_index(name) for name in COL)
    rows, cols, count = block_rows[0, 0], block_cols[0, 0], counts[0]
    live = jnp.arange(rows.shape[0], dtype=jnp.int32) < count[0]
    owner, within = rows // 8, rows % 8
    to_z, away = owner // 2, jnp.bitwise_xor(owner % 2, yl)
    early_row = 16 * LATE + (to_z * 2 + away) * EARLY + within - LATE
    late_row = (away * 8 + (to_z - z) % 8) * LATE + within
    rows = jnp.where(within < LATE, late_row, early_row)
    holder = cols // 8
    distance = (
        jnp.bitwise_xor(holder // 8, yh) * 8 + ((holder // 2 - x) % 4) * 2 + jnp.bitwise_xor(holder % 2, c)
    )
    packed = sort_slots(rows, distance * 8 + cols % 8, live, rows.shape[0] + 2 * GROUP)
    pieces, places = gather_panel(features.reshape(-1, bs, width))
    early, *parts = tile_product(
        blocks[0, 0], packed, count, c.reshape(1), pieces, places
    )
    early = lax.psum_scatter(early, "z", scatter_dimension=0, tiled=True)

    sent, kept = parts[: 2 * HOPS + 1], parts[2 * HOPS + 1 :]
    joined = []
    for hop in range(HOPS):
        mine = flip(sent[hop], ("yl",))
        theirs = flip(sent[HOPS + hop], ("c", "yl"))
        kept_theirs = flip(kept[HOPS + hop], ("c",))
        joined.append(lax.optimization_barrier(jnp.stack([kept[hop] + mine, kept_theirs + theirs])))
    near = flip(sent[2 * HOPS], ("yl",))
    around = [(i, (i + 1) % 8) for i in range(8)] + [(8 + i, 8 + (i - 1) % 8) for i in range(8)]
    moving = joined[0]
    for hop in range(HOPS):
        moving = lax.ppermute(moving, ("c", "z"), around)
        if hop == HOPS - 1:
            break
        if hop == 0:
            below = jnp.pad(moving, ((0, 0), (LATE // 2, 0), (0, 0), (0, 0)))
            above = jnp.pad(moving, ((0, 0), (0, LATE // 2), (0, 0), (0, 0)))
            moving = jnp.where(c == 0, below, above)
        moving = joined[hop + 1] + moving
    other_side = flip(moving[1], ("c",))
    last = flip(early[EARLY:], ("yl",))
    late = moving[0] + other_side + (kept[2 * HOPS] + near)
    return jnp.concatenate([late, early[:EARLY] + last], 0).reshape(-1, width)


def solution(mesh):
    finer = Mesh(mesh.devices.reshape(2, 4, 2, 8, 2), ROW + COL)
    placed = (
        P(ROW, COL, None, None, None),
        P(ROW, COL, None),
        P(ROW, COL, None),
        P(ROW, COL),
        P(COL + ROW, None),
    )

    return jax.shard_map(on_device, mesh=finer, in_specs=placed, out_specs=P(ROW + COL, None), check_vma=False)
```

```python
import jax
import jax.numpy as jnp
from jax import lax
from jax.experimental import pallas as pl
from jax.experimental.pallas import tpu as pltpu
from jax.sharding import Mesh
from jax.sharding import PartitionSpec as P


ROW = ("yh", "x", "c")
COL = ("z", "yl")
GROUP = 16
BUFFERS = 4
LATE = 4
EARLY = 8 - LATE
HOPS = 4


def shift(array, axis, step):
    n = lax.axis_size(axis)
    return lax.ppermute(array, axis, [(i, (i + step) % n) for i in range(n)])


def tile_product(blocks, packed, count, core, pieces, places):
    bs, width = pieces[0].shape[1:]
    n_pieces, n_cols, n_rows = len(pieces), 128, 128
    late_rows, part_rows = 16 * LATE, 8
    late_parts, parts = late_rows // part_rows, n_rows // part_rows
    lates = []
    for row, unit in ((8 * LATE, LATE), (0, LATE), (late_rows, 2 * EARLY)):
        for other in range(2):
            lates += [(row, unit, other, hop, unit if hop else unit // 2) for hop in range(HOPS)]
        lates.append((row, unit, None, 0, unit))
    n_late = 2 * (2 * HOPS + 1)
    shapes = [(n, bs, width) for *_, n in lates]

    def body(count_ref, core_ref, packed_ref, blocks_ref, *rest):
        piece_refs = rest[:n_pieces]
        late_refs = rest[n_pieces : n_pieces + len(lates)]
        acc, panel, weights, *rest = rest[n_pieces + len(lates) :]
        late_staged, (piece_sem, weight_sem, late_sem) = rest[: len(lates)], rest[len(lates) :]
        groups = (count_ref[0] + GROUP - 1) // GROUP

        def weight_copies(group):
            slot = lax.rem(group, BUFFERS)
            return [
                pltpu.make_async_copy(
                    blocks_ref.at[packed_ref[group * GROUP + i] & 511],
                    weights.at[slot, i],
                    weight_sem.at[slot, i],
                )
                for i in range(GROUP)
            ]

        def fetch(group):
            @pl.when(group < groups)
            def _():
                for copy in weight_copies(group):
                    copy.start()

        piece_copies = [
            pltpu.make_async_copy(ref, panel.at[pl.ds(place, piece.shape[0])], piece_sem.at[i])
            for i, (ref, piece, place) in enumerate(zip(piece_refs, pieces, places))
        ]
        for copy in piece_copies:
            copy.start()
        for group in range(BUFFERS - 1):
            fetch(group)

        def clear(i, _):
            acc[i] = jnp.zeros((bs, width), jnp.float32)
            return 0

        lax.fori_loop(0, n_rows + 1, clear, 0)
        for copy in piece_copies:
            copy.wait()

        def late_copy(i):
            return pltpu.make_async_copy(late_staged[i], late_refs[i], late_sem.at[i])

        def write_some(chosen):
            for i in chosen:
                row, unit, other, hop, n = lates[i]
                if other is None:
                    distance = skip = 0
                else:
                    down = 1 - core_ref[0] if other else core_ref[0]
                    distance = 4 + hop * (2 * down - 1)
                    skip = 0 if hop else (1 - down) * (unit // 2)

                def one_row(k, _, i=i, first=row + distance * unit + skip):
                    late_staged[i][k] = acc[first + k].astype(jnp.bfloat16)
                    return 0

                lax.fori_loop(0, n, one_row, 0)
                late_copy(i).start()

        def write(part, _):
            @pl.when(part == late_parts - 1)
            def _():
                write_some(range(n_late))

            @pl.when(part == parts - 1)
            def _():
                write_some(range(n_late, len(lates)))

            return 0

        def one_group(group, finished):
            slot = lax.rem(group, BUFFERS)
            fetch(group + BUFFERS - 1)
            for copy in weight_copies(group):
                copy.wait()
            for i in range(GROUP):
                entry = packed_ref[group * GROUP + i]
                row = 128 - (entry >> 16)
                col = (entry >> 9) & 127
                acc[row] += jnp.dot(weights[slot, i], panel[col], preferred_element_type=jnp.float32)
            ready = (128 - (packed_ref[(group + 1) * GROUP] >> 16)) // part_rows
            lax.fori_loop(finished, ready, write, 0)
            return ready

        finished = lax.fori_loop(0, groups, one_group, 0)
        lax.fori_loop(finished, parts, write, 0)
        for i in range(len(lates)):
            late_copy(i).wait()

    anywhere = pl.BlockSpec(memory_space=pl.ANY)
    hbm = pl.BlockSpec(memory_space=pltpu.MemorySpace.HBM)
    smem = pl.BlockSpec(memory_space=pltpu.SMEM)
    return pl.pallas_call(
        body,
        out_shape=[jax.ShapeDtypeStruct(shape, jnp.bfloat16) for shape in shapes],
        in_specs=[smem, smem, smem, hbm] + [anywhere] * n_pieces,
        out_specs=[anywhere] * len(lates),
        scratch_shapes=[
            pltpu.VMEM((n_rows + 1, bs, width), jnp.float32),
            pltpu.VMEM((n_cols, bs, width), jnp.bfloat16),
            pltpu.VMEM((BUFFERS, GROUP, bs, bs), jnp.bfloat16),
            *[pltpu.VMEM(shape, jnp.bfloat16) for shape in shapes],
            pltpu.SemaphoreType.DMA((n_pieces,)),
            pltpu.SemaphoreType.DMA((BUFFERS, GROUP)),
            pltpu.SemaphoreType.DMA((len(lates),)),
        ],
        compiler_params=pltpu.CompilerParams(vmem_limit_bytes=59 * 2**20),
        cost_estimate=pl.CostEstimate(
            flops=n_rows * 3 * 2 * bs * bs * width, bytes_accessed=30 * 2**20, transcendentals=0
        ),
        name="tile_product",
    )(count, core, packed, blocks, *pieces)


def gather_panel(own):
    half = own.shape[0] // 2
    got = [(own, 0, 0, 0)]
    across = shift(own, "yh", 1)
    got.append((across, 1, 0, 0))
    for part, dyh in ((own, 0), (across, 1)):
        before = shift(part, "x", 1)
        after = shift(part, "x", -1)
        far_low = shift(before[:half], "x", 1)
        far_high = shift(after[half:], "x", -1)
        got += [(before, dyh, 3, 0), (after, dyh, 1, 0), (far_low, dyh, 2, 0), (far_high, dyh, 2, half)]
    pieces, places = [], []
    for part, dyh, dx, at in got:
        for dc in range(2):
            pieces.append(shift(part, "c", 1) if dc else part)
            places.append(((dyh * 4 + dx) * 2 + dc) * 8 + at)
    return pieces, places


def sort_slots(rows, cols, live, total):
    slots = jnp.arange(rows.shape[0], dtype=jnp.int32)
    key = jnp.where(live, rows, 128) * 512 + slots
    rank = jnp.sum((key[None, :] < key[:, None]).astype(jnp.int32), axis=1)
    entry = jnp.where(live, slots + 512 * cols + 65536 * (128 - rows), 0)
    places = jnp.arange(total, dtype=jnp.int32)
    picked = jnp.where(rank[:, None] == places[None, :], entry[:, None], 0)
    return jnp.sum(picked, axis=0)


def flip(array, axes):
    n = 2 ** len(axes)
    return lax.ppermute(array, axes, [(i, n - 1 - i) for i in range(n)])


def on_device(blocks, block_rows, block_cols, counts, features):
    bs = blocks.shape[-1]
    width = features.shape[1]
    yh, x, c = (lax.axis_index(name) for name in ROW)
    z, yl = (lax.axis_index(name) for name in COL)
    rows, cols, count = block_rows[0, 0], block_cols[0, 0], counts[0]
    live = jnp.arange(rows.shape[0], dtype=jnp.int32) < count[0]
    owner, within = rows // 8, rows % 8
    to_z, away = owner // 2, jnp.bitwise_xor(owner % 2, yl)
    early_row = 16 * LATE + ((to_z - z) % 8 * 2 + away) * EARLY + within - LATE
    late_row = (away * 8 + (to_z - z) % 8) * LATE + within
    rows = jnp.where(within < LATE, late_row, early_row)
    holder = cols // 8
    distance = (
        jnp.bitwise_xor(holder // 8, yh) * 8 + ((holder // 2 - x) % 4) * 2 + jnp.bitwise_xor(holder % 2, c)
    )
    packed = sort_slots(rows, distance * 8 + cols % 8, live, rows.shape[0] + 2 * GROUP)
    pieces, places = gather_panel(features.reshape(-1, bs, width))
    parts = tile_product(
        blocks[0, 0], packed, count, c.reshape(1), pieces, places
    )
    n = 2 * HOPS + 1
    sent, kept, early = parts[:n], parts[n : 2 * n], parts[2 * n :]
    joined = []
    for hop in range(HOPS):
        mine = flip(sent[hop], ("yl",))
        theirs = flip(sent[HOPS + hop], ("c", "yl"))
        kept_theirs = flip(kept[HOPS + hop], ("c",))
        joined.append(lax.optimization_barrier(jnp.stack([kept[hop] + mine, kept_theirs + theirs])))
    near = flip(sent[2 * HOPS], ("yl",))
    merged = []
    for hop in range(HOPS):
        theirs = flip(early[HOPS + hop], ("c",))
        merged.append(lax.optimization_barrier(jnp.stack([early[hop], theirs])))
    around = [(i, (i + 1) % 8) for i in range(8)] + [(8 + i, 8 + (i - 1) % 8) for i in range(8)]

    def widened(array):
        half = array.shape[1]
        below = jnp.pad(array, ((0, 0), (half, 0), (0, 0), (0, 0)))
        above = jnp.pad(array, ((0, 0), (0, half), (0, 0), (0, 0)))
        return jnp.where(c == 0, below, above)

    moving, large = joined[0], merged[0]
    for hop in range(HOPS):
        large = lax.ppermute(large, ("c", "z"), around)
        moving = lax.ppermute(moving, ("c", "z"), around)
        if hop < HOPS - 1:
            large = merged[hop + 1] + (large if hop else widened(large))
            moving = joined[hop + 1] + (moving if hop else widened(moving))
    large = large[0] + flip(large[1], ("c",)) + early[2 * HOPS]
    last = flip(large[EARLY:], ("yl",))
    other_side = flip(moving[1], ("c",))
    late = moving[0] + other_side + (kept[2 * HOPS] + near)
    return jnp.concatenate([late, large[:EARLY] + last], 0).reshape(-1, width)


def solution(mesh):
    finer = Mesh(mesh.devices.reshape(2, 4, 2, 8, 2), ROW + COL)
    placed = (
        P(ROW, COL, None, None, None),
        P(ROW, COL, None),
        P(ROW, COL, None),
        P(ROW, COL),
        P(COL + ROW, None),
    )

    return jax.shard_map(on_device, mesh=finer, in_specs=placed, out_specs=P(ROW + COL, None), check_vma=False)
```
